32 devices in a mesh: lat: 16 (over z, y, core), ch: 2 (over x).
Axes of the slice: x: 2, y: 2, z: 4, core: 2. Of those that a mesh axis runs over, the one named last changes fastest.
Arguments:
- tokens: bfloat16 [16, 64, 138240], P(None, 'lat', 'ch'), may hold values from -60 to 60
- norm_gain: float32 [768], P('ch'), may hold values from 0.25 to 1.75
- norm_shift: float32 [768], P('ch'), may hold values from -1.5 to 1.5
- first_weight: float32 [2, 8, 96, 96], P(None, 'ch'), may hold values from -0.625 to 0.625
- first_bias: float32 [2, 8, 96], P(None, 'ch'), may hold values from -1.5 to 1.5
- second_weight: float32 [2, 8, 96, 96], P(None, 'ch'), may hold values from -0.625 to 0.625
- second_bias: float32 [2, 8, 96], P(None, 'ch'), may hold values from -1.5 to 1.5
- upstream: bfloat16 [16, 64, 138240], P(None, 'lat', 'ch'), may hold values from -6 to 6
Outputs:
- result: bfloat16 [16, 64, 138240], P(None, 'lat', 'ch')
- grad_tokens: bfloat16 [16, 64, 138240], P(None, 'lat', 'ch')
- grad_first_weight: float32 [2, 8, 96, 96], P(None, 'ch')
- grad_first_bias: float32 [2, 8, 96], P(None, 'ch')
- grad_second_weight: float32 [2, 8, 96, 96], P(None, 'ch')
- grad_second_bias: float32 [2, 8, 96], P(None, 'ch')
- grad_norm_gain: float32 [768], P('ch')
- grad_norm_shift: float32 [768], P('ch')
The draws below stay inside these ranges and needn't reach their ends.
All inputs are finite; a program needn't handle non-finite values.
Results may differ from the reference program's by a relative error of at most 0.0086.
Values may be sent and summed in bfloat16 or wider, within the bound.
A program may use at most 384 MiB of HBM per device.

```python
import math
import jax
import jax.numpy as jnp
from jax import lax

EMBED = 768
BLOCKS = 8
LON = 180
LAT_CELLS = 64
BATCH = 16
BLOCK = 96


def draw_tokens(key, part):
    base_key = jax.random.fold_in(key, 7)
    key_list = jax.random.split(base_key, 4)
    dims_shape = (BATCH, LAT_CELLS, LON, EMBED)
    channel_index = jnp.arange(EMBED, dtype=jnp.float32)
    channel_scale = 0.6 * jnp.exp(math.log(3.0) * channel_index / max(EMBED - 1, 1))
    channel_scale = channel_scale * jnp.exp(jax.random.uniform(key_list[0], (EMBED,), jnp.float32, math.log(0.5), math.log(2.0)))
    token_scale = jnp.exp(jax.random.uniform(key_list[1], (BATCH, LAT_CELLS, LON, 1), jnp.float32, math.log(0.3), math.log(3.0)))
    values = jnp.clip(jax.random.normal(key_list[3], dims_shape, jnp.float32), -5.0, 5.0)
    field_out = values * channel_scale * token_scale
    return jnp.transpose(field_out, (0, 1, 3, 2)).reshape(BATCH, LAT_CELLS, EMBED * LON).astype(jnp.bfloat16)


def level_of(stream_key, dims, shards, smallest, largest):
    def one(axis_at, blocks):
        draws = jax.random.uniform(jax.random.fold_in(jax.random.fold_in(stream_key, 6), axis_at), (blocks,), jnp.float32, smallest / len(shards), largest / len(shards))
        return jnp.repeat(jnp.exp(draws), dims[axis_at] // blocks).reshape((-1,) + (1,) * (len(dims) - axis_at - 1))

    level = one(*shards[0])
    for cut in shards[1:]:
        level = level * one(*cut)
    return level


def gaussian(stream_key, extent, spread, limit, cuts=(), held_as=jnp.bfloat16):
    values = jax.random.normal(stream_key, extent, jnp.float32) * spread
    if len(cuts) > 0:
        values = level_of(stream_key, extent, cuts, -0.22, 0.18) * values
    return jnp.clip(values, min=-limit, max=limit).astype(held_as)


def setup_inputs(seed: int = 0) -> dict:
    key_of = jax.random.split(jax.random.key(seed), 9)
    tokens = draw_tokens(jax.random.fold_in(key_of[8], 71), 0)
    norm_gain = jnp.clip(1.0 + 0.15 * jax.random.normal(key_of[1], (EMBED,), jnp.float32), 0.25, 1.75)
    norm_shift = gaussian(key_of[2], (EMBED,), 0.3, 1.5, ((0, 2),), jnp.float32)
    first_weight = gaussian(key_of[3], (2, BLOCKS, BLOCK, BLOCK), BLOCK ** -0.5, 0.625, ((1, 2),), jnp.float32)
    first_bias = gaussian(key_of[4], (2, BLOCKS, BLOCK), 0.3, 1.5, ((1, 2),), jnp.float32)
    second_weight = gaussian(key_of[5], (2, BLOCKS, BLOCK, BLOCK), BLOCK ** -0.5, 0.625, ((1, 2),), jnp.float32)
    second_bias = gaussian(key_of[6], (2, BLOCKS, BLOCK), 0.3, 1.5, ((1, 2),), jnp.float32)
    upstream = gaussian(key_of[7], (BATCH, LAT_CELLS, EMBED * LON), 1.0, 6.0, ((1, 16), (2, 2)))
    return dict(tokens=tokens, norm_gain=norm_gain, norm_shift=norm_shift, first_weight=first_weight, first_bias=first_bias, second_weight=second_weight, second_bias=second_bias, upstream=upstream)


layer_eps = 1e-05
shrink_level = 0.1
highest = lax.Precision.HIGHEST

def block_mix(values, matrix):
    return jnp.einsum('bhknc,ncd->bhknd', values, matrix, precision=highest)

def smooth_gelu(values):
    return 0.5 * values * (1.0 + jnp.tanh(math.sqrt(2.0 / math.pi) * (values + 0.044715 * values * values * values)))

def spectral_mlp(real_part, imag_part, params):
    first_weight, first_bias, second_weight, second_bias = params
    dims_shape = real_part.shape
    groups = first_weight.shape[1]
    block_width = first_weight.shape[2]
    real_part = real_part.reshape(dims_shape[:-1] + (groups, block_width))
    imag_part = imag_part.reshape(dims_shape[:-1] + (groups, block_width))
    hidden_real = smooth_gelu(block_mix(real_part, first_weight[0]) - block_mix(imag_part, first_weight[1]) + first_bias[0])
    hidden_imag = smooth_gelu(block_mix(imag_part, first_weight[0]) + block_mix(real_part, first_weight[1]) + first_bias[1])
    mixed_real = block_mix(hidden_real, second_weight[0]) - block_mix(hidden_imag, second_weight[1]) + second_bias[0]
    mixed_imag = block_mix(hidden_imag, second_weight[0]) + block_mix(hidden_real, second_weight[1]) + second_bias[1]
    mixed_real = mixed_real - shrink_level * jnp.tanh(mixed_real / shrink_level)
    mixed_imag = mixed_imag - shrink_level * jnp.tanh(mixed_imag / shrink_level)
    return (mixed_real.reshape(dims_shape), mixed_imag.reshape(dims_shape))

def spectral_filter(field_in, params):
    spectrum = jnp.fft.rfft2(field_in, axes=(1, 2), norm='ortho')
    mixed_real, mixed_imag = spectral_mlp(jnp.real(spectrum), jnp.imag(spectrum), params)
    return jnp.fft.irfft2(mixed_real + 1j * mixed_imag, s=(LAT_CELLS, LON), axes=(1, 2), norm='ortho')

def unmerge(sample):
    return jnp.transpose(sample.reshape(LAT_CELLS, EMBED, LON), (0, 2, 1))

def merge(field_in):
    return jnp.transpose(field_in, (0, 2, 1)).reshape(LAT_CELLS, EMBED * LON)

def reference(tokens, norm_gain, norm_shift, first_weight, first_bias, second_weight, second_bias, upstream):
    params = (first_weight, first_bias, second_weight, second_bias)
    initial = (jnp.zeros_like(first_weight), jnp.zeros_like(first_bias), jnp.zeros_like(second_weight), jnp.zeros_like(second_bias), jnp.zeros_like(norm_gain), jnp.zeros_like(norm_shift))

    def per_sample(carry, items):
        sample, cotangent = items
        as_float = unmerge(sample).astype(jnp.float32)[None]
        totals = lax.optimization_barrier(jnp.sum(as_float, axis=-1, keepdims=True))
        squares = lax.optimization_barrier(jnp.sum(as_float * as_float, axis=-1, keepdims=True))
        center = totals / EMBED
        variance = squares / EMBED - center * center
        inv_scale = lax.rsqrt(variance + layer_eps)
        standard = (as_float - center) * inv_scale
        normed = lax.optimization_barrier((standard * norm_gain + norm_shift).astype(jnp.bfloat16))
        normed_float = normed.astype(jnp.float32)
        filtered_float, pullback = jax.vjp(spectral_filter, normed_float, params)
        filtered = lax.optimization_barrier(filtered_float.astype(jnp.bfloat16))
        result = (as_float + normed_float + filtered.astype(jnp.float32)).astype(jnp.bfloat16)
        grad_out = unmerge(cotangent).astype(jnp.float32)[None]
        field_grad, param_grads = pullback(grad_out)
        spectral_grad = lax.optimization_barrier(field_grad.astype(jnp.bfloat16))
        normed_grad = grad_out + spectral_grad.astype(jnp.float32)
        gain_part = lax.optimization_barrier(jnp.sum(normed_grad * standard, axis=(0, 1, 2)))
        shift_part = lax.optimization_barrier(jnp.sum(normed_grad, axis=(0, 1, 2)))
        standard_grad = normed_grad * norm_gain
        grad_mean = lax.optimization_barrier(jnp.sum(standard_grad, axis=-1, keepdims=True)) / EMBED
        grad_cross = lax.optimization_barrier(jnp.sum(standard_grad * standard, axis=-1, keepdims=True)) / EMBED
        grad_tokens = (grad_out + inv_scale * (standard_grad - grad_mean - standard * grad_cross)).astype(jnp.bfloat16)
        updated = (carry[0] + param_grads[0], carry[1] + param_grads[1], carry[2] + param_grads[2], carry[3] + param_grads[3], carry[4] + gain_part, carry[5] + shift_part)
        return (updated, (merge(result[0]), merge(grad_tokens[0])))
    totals_out, (result, grad_tokens) = lax.scan(per_sample, initial, (tokens, upstream))
    return (result, grad_tokens, totals_out[0], totals_out[1], totals_out[2], totals_out[3], totals_out[4], totals_out[5])
```

```python
import functools
import math

import jax
import jax.numpy as jnp
import numpy as np
from jax import lax
from jax.experimental import pallas as pl
from jax.experimental.pallas import tpu as pltpu
from jax.sharding import PartitionSpec as P

layer_eps = 1e-05
shrink_level = 0.1
LANE = 128
PAD = 256
F32 = jnp.float32
BF16 = jnp.bfloat16
GELU_SCALE = math.sqrt(2.0 / math.pi)
GELU_CUBE = 0.044715
VMEM_BYTES = 60 * 1024 * 1024


def split_table(table):
    full = jnp.asarray(table, F32)
    high = lax.reduce_precision(full, 8, 7)
    return high.astype(BF16), (full - high).astype(BF16)


def left_table(table, passes):
    high, low = split_table(table)
    return jnp.concatenate((high, high, low)[:passes] if passes != 2 else (high, low), axis=1)


def right_table(table, passes):
    high, low = split_table(table)
    return jnp.concatenate((high, high, low)[:passes] if passes != 2 else (high, low), axis=0)


def latitude_table(height):
    cells = np.arange(height)
    table = np.zeros((height, height))
    for pair in range(height // 2):
        angle = 2.0 * np.pi * (pair * cells % height) / height
        table[2 * pair] = np.cos(angle)
        table[2 * pair + 1] = -np.sin(angle)
    table[1] = np.cos(np.pi * cells)
    return table


def longitude_table(width):
    modes = width // 2 + 1
    cells = np.arange(width)[:, None]
    angle = 2.0 * np.pi * (cells * np.arange(modes)[None] % width) / width
    table = np.zeros((PAD, PAD))
    table[:width, :modes] = np.cos(angle)
    table[:width, LANE : LANE + modes] = -np.sin(angle)
    doubled = np.full((modes,), 2.0)
    doubled[0] = 1.0
    if width % 2 == 0:
        doubled[-1] = 1.0
    weights = np.zeros((PAD,))
    weights[:modes] = doubled
    weights[LANE : LANE + modes] = doubled
    return table, table * weights[None]


def dot(left, right):
    return jnp.dot(left, right, preferred_element_type=F32)


def dot_rows(left, right):
    return lax.dot_general(left, right, (((1,), (1,)), ((), ())), preferred_element_type=F32)


def pair_forward(values, first, half):
    real_cos = values[:half, :LANE]
    real_sin = values[:half, LANE:]
    imag_cos = values[half:, :LANE]
    imag_sin = values[half:, LANE:]
    re_left = jnp.where(first, real_cos, real_cos - imag_sin)
    re_right = jnp.where(first, imag_cos, real_cos + imag_sin)
    im_left = jnp.where(first, real_sin, imag_cos + real_sin)
    im_right = jnp.where(first, imag_sin, real_sin - imag_cos)
    top = jnp.concatenate((re_left, re_right), axis=1)
    bottom = jnp.concatenate((im_left, im_right), axis=1)
    return jnp.concatenate((top, bottom), axis=0)


def pair_inverse(values, first, half):
    re_left = values[:half, :LANE]
    re_right = values[:half, LANE:]
    im_left = values[half:, :LANE]
    im_right = values[half:, LANE:]
    a = jnp.where(first, re_left, re_left + re_right)
    b = jnp.where(first, im_left, im_left + im_right)
    c = jnp.where(first, re_right, im_left - im_right)
    d = jnp.where(first, im_right, re_right - re_left)
    top = jnp.concatenate((a, b), axis=1)
    bottom = jnp.concatenate((c, d), axis=1)
    return jnp.concatenate((top, bottom), axis=0)


def split(values):
    high = values.astype(BF16)
    return high, (values - high.astype(F32)).astype(BF16)


def to_modes(x_ref, lat_ref, flat, low, high, group, width, block):
    height = x_ref.shape[0]
    span = group * width
    flat[:, span:] = jnp.zeros((height, flat.shape[1] - span), F32)

    def one(step, carry):
        at = pl.multiple_of(step * span, LANE)
        piece = x_ref[:, pl.ds(at, span)]
        if lat_ref.shape[1] == 2 * height:
            piece = jnp.concatenate((piece, piece), axis=0)
        flat[:, :span] = dot(lat_ref[...], piece)
        for channel in range(group):
            start = channel * width
            rows = pl.ds(step * group + channel, height, stride=block)
            low[rows, :] = flat[:, start : start + LANE]
            high[rows, :] = flat[:, start + LANE : start + PAD]
        return carry

    lax.fori_loop(0, block // group, one, 0)


def from_modes(out_ref, lat_ref, flat, low, high, group, width, block):
    height = out_ref.shape[0]
    span = group * width

    def one(step, carry):
        at = pl.multiple_of(step * span, LANE)
        for channel in range(group):
            start = channel * width
            rows = pl.ds(step * group + channel, height, stride=block)
            flat[:, start : start + LANE] = low[rows, :]
            flat[:, start + LANE : start + PAD] = high[rows, :]
        piece = flat[:, :span].astype(BF16)
        out = dot(lat_ref[...], piece) * (1.0 / math.sqrt(height * width))
        out_ref[:, pl.ds(at, span)] = out.astype(BF16)
        return carry

    lax.fori_loop(0, block // group, one, 0)


def load_rows(low, high, rows):
    return jnp.concatenate((low[rows, :], high[rows, :]), axis=1)


def forward_kernel(
    group, width, block, unroll, x_ref, lat_ref, lat_back_ref, lon_ref, lon_back_ref, first_ref,
    first_bias_ref, second_ref, second_bias_ref, out_ref, spec_ref, slope_ref, hidden_ref,
    shrink_ref, flat, low, high,
):
    height = x_ref.shape[0]
    to_modes(x_ref, lat_ref, flat, low, high, group, width, block)
    two = 2 * block

    def one(step, carry):
        rows = pl.ds(pl.multiple_of(step * (unroll * two), 8), unroll * two)
        major, minor = split(load_rows(low, high, rows))
        modes = dot(jnp.concatenate((major, minor, major), axis=1), lon_ref[...])
        backs = []
        for index in range(unroll):
            pair = step * unroll + index
            first = pair == 0
            major, minor = split(pair_forward(modes[index * two : (index + 1) * two], first, block))
            spec_ref[0, pair] = major
            pre = dot(first_ref[0], jnp.concatenate((major, minor, major), axis=0))
            pre = pre + first_bias_ref[0]
            square = pre * pre
            inner = jnp.tanh(GELU_SCALE * (pre + GELU_CUBE * square * pre))
            half = 0.5 * (1.0 + inner)
            slope = half + 0.5 * GELU_SCALE * pre * (1.0 - inner * inner) * (
                1.0 + 3.0 * GELU_CUBE * square
            )
            slope_ref[0, pair] = slope.astype(BF16)
            major, minor = split(pre * half)
            hidden_ref[0, pair] = major
            mixed = dot(second_ref[0], jnp.concatenate((major, minor, major), axis=0))
            mixed = mixed + second_bias_ref[0]
            shrink = jnp.tanh(mixed / shrink_level)
            shrink_ref[0, pair] = (shrink * shrink).astype(BF16)
            mixed = mixed - shrink_level * shrink
            backs.append(pair_inverse(mixed, first, block).astype(BF16))
        back = dot(jnp.concatenate(backs, axis=0), lon_back_ref[...])
        low[rows, :] = back[:, :LANE]
        high[rows, :] = back[:, LANE:]
        return carry

    lax.fori_loop(0, height // (2 * unroll), one, 0)
    from_modes(out_ref, lat_back_ref, flat, low, high, group, width, block)


def backward_kernel(
    group, width, block, unroll, x_ref, spec_ref, slope_ref, hidden_ref, shrink_ref, lat_ref,
    lat_back_ref, lon_ref, lon_back_ref, first_ref, second_ref, out_ref, first_grad_ref,
    first_bias_grad_ref, second_grad_ref, second_bias_grad_ref, flat, low, high,
):
    height = x_ref.shape[0]
    to_modes(x_ref, lat_ref, flat, low, high, group, width, block)
    two = 2 * block
    first_grad_ref[...] = jnp.zeros_like(first_grad_ref)
    second_grad_ref[...] = jnp.zeros_like(second_grad_ref)
    first_bias_grad_ref[...] = jnp.zeros_like(first_bias_grad_ref)
    second_bias_grad_ref[...] = jnp.zeros_like(second_bias_grad_ref)

    def one(step, carry):
        rows = pl.ds(pl.multiple_of(step * (unroll * two), 8), unroll * two)
        modes = dot(load_rows(low, high, rows).astype(BF16), lon_ref[...])
        backs = []
        grads = []
        for index in range(unroll):
            pair = step * unroll + index
            first = pair == 0
            grad = pair_forward(modes[index * two : (index + 1) * two], first, block)
            outer = grad * shrink_ref[0, pair].astype(F32)
            outer_low = outer.astype(BF16)
            inner = dot(second_ref[0], outer_low) * slope_ref[0, pair].astype(F32)
            inner_low = inner.astype(BF16)
            back = pair_inverse(dot(first_ref[0], inner_low), first, block)
            backs.append(back.astype(BF16))
            grads.append((outer, outer_low, inner, inner_low))
        hiddens = jnp.concatenate([hidden_ref[0, step * unroll + i] for i in range(unroll)], axis=1)
        specs = jnp.concatenate([spec_ref[0, step * unroll + i] for i in range(unroll)], axis=1)
        outers = jnp.concatenate([grad[1] for grad in grads], axis=1)
        inners = jnp.concatenate([grad[3] for grad in grads], axis=1)
        second_grad_ref[0] += dot_rows(outers, hiddens)
        first_grad_ref[0] += dot_rows(inners, specs)
        outer_sum = sum(grad[0][:, :LANE] + grad[0][:, LANE:] for grad in grads)
        inner_sum = sum(grad[2][:, :LANE] + grad[2][:, LANE:] for grad in grads)
        second_bias_grad_ref[0] += outer_sum
        first_bias_grad_ref[0] += inner_sum
        back = dot(jnp.concatenate(backs, axis=0), lon_back_ref[...])
        low[rows, :] = back[:, :LANE]
        high[rows, :] = back[:, LANE:]
        return carry

    lax.fori_loop(0, height // (2 * unroll), one, 0)
    from_modes(out_ref, lat_back_ref, flat, low, high, group, width, block)


def whole(array):
    rank = array.ndim
    return pl.BlockSpec(array.shape, lambda *_: (0,) * rank)


def per_block(shape, offset=0):
    rank = len(shape)
    return pl.BlockSpec((1,) + tuple(shape), lambda n: (n + offset,) + (0,) * rank)


def column_scratch(height, group, width, block):
    return [
        pltpu.VMEM((height, group * width + LANE), F32),
        pltpu.VMEM((height * block, LANE), F32),
        pltpu.VMEM((height * block, LANE), F32),
    ]


def column_forward(x, tables, params, group, width, block, start, unroll=4):
    height, lanes = x.shape
    blocks = lanes // (block * width)
    pairs = height // 2
    two = 2 * block
    wide = pl.BlockSpec((height, block * width), lambda n: (0, n))
    kept = per_block((pairs, two, PAD))
    cells = blocks * pairs * two * PAD
    return pl.pallas_call(
        functools.partial(forward_kernel, group, width, block, unroll),
        grid=(blocks,),
        in_specs=[
            wide, *[whole(table) for table in tables],
            per_block((two, 3 * two), start), per_block((two, 1), start),
            per_block((two, 3 * two), start), per_block((two, 1), start),
        ],
        out_specs=[wide] + [kept] * 4,
        out_shape=[jax.ShapeDtypeStruct(x.shape, BF16)]
        + [jax.ShapeDtypeStruct((blocks, pairs, two, PAD), BF16)] * 4,
        scratch_shapes=column_scratch(height, group, width, block),
        compiler_params=pltpu.CompilerParams(vmem_limit_bytes=VMEM_BYTES),
        cost_estimate=pl.CostEstimate(
            flops=cells * 20000, bytes_accessed=4 * height * lanes + 8 * cells, transcendentals=0
        ),
        name="column_forward",
    )(x, *tables, *params)


def column_backward(x, kept_arrays, tables, params, group, width, block, start, local, unroll=4):
    height, lanes = x.shape
    blocks = lanes // (block * width)
    pairs = height // 2
    two = 2 * block
    wide = pl.BlockSpec((height, block * width), lambda n: (0, n))
    kept = per_block((pairs, two, PAD), local)
    cells = blocks * pairs * two * PAD
    sizes = ((two, two), (two, LANE)) * 2
    return pl.pallas_call(
        functools.partial(backward_kernel, group, width, block, unroll),
        grid=(blocks,),
        in_specs=[
            wide, kept, kept, kept, kept, *[whole(table) for table in tables],
            per_block((two, two), start), per_block((two, two), start),
        ],
        out_specs=[wide] + [per_block(size) for size in sizes],
        out_shape=[jax.ShapeDtypeStruct(x.shape, BF16)]
        + [jax.ShapeDtypeStruct((blocks,) + size, F32) for size in sizes],
        scratch_shapes=column_scratch(height, group, width, block),
        compiler_params=pltpu.CompilerParams(vmem_limit_bytes=VMEM_BYTES),
        cost_estimate=pl.CostEstimate(
            flops=cells * 20000, bytes_accessed=4 * height * lanes + 8 * cells, transcendentals=0
        ),
        name="column_backward",
    )(x, *kept_arrays, *tables, *params)


def fold(acc, group, width):
    total = acc[:, :width]
    for channel in range(1, group):
        total = total + acc[:, channel * width : (channel + 1) * width]
    return total


def spread(wide, token, group, width):
    for channel in range(group):
        wide[:, channel * width : (channel + 1) * width] = token


def each_group(groups, span, step_body):
    def one(step, carry):
        step_body(pl.ds(pl.multiple_of(step * span, LANE), span))
        return carry

    lax.fori_loop(0, groups, one, 0)


def stats_kernel(group, width, x_ref, total_ref, square_ref, acc, acc_square):
    span = group * width
    acc[...] = jnp.zeros_like(acc)
    acc_square[...] = jnp.zeros_like(acc_square)

    def one(at):
        piece = x_ref[0, :, at].astype(F32)
        acc[...] += piece
        acc_square[...] += piece * piece

    each_group(x_ref.shape[2] // span, span, one)
    total_ref[0] = fold(acc, group, width)
    square_ref[0] = fold(acc_square, group, width)


def norm_kernel(group, width, x_ref, center_ref, inv_ref, gain_ref, shift_ref, out_ref, center, inv):
    span = group * width
    spread(center, center_ref[0], group, width)
    spread(inv, inv_ref[0], group, width)

    def one(at):
        standard = (x_ref[0, :, at].astype(F32) - center[...]) * inv[...]
        out_ref[0, :, at] = (standard * gain_ref[:, at] + shift_ref[:, at]).astype(BF16)

    each_group(x_ref.shape[2] // span, span, one)


def sums_kernel(
    group, width, x_ref, up_ref, grad_ref, center_ref, inv_ref, gain_ref,
    mean_ref, cross_ref, gain_grad_ref, shift_grad_ref, center, inv, acc, acc_cross,
):
    span = group * width
    spread(center, center_ref[0], group, width)
    spread(inv, inv_ref[0], group, width)
    acc[...] = jnp.zeros_like(acc)
    acc_cross[...] = jnp.zeros_like(acc_cross)

    @pl.when(pl.program_id(0) == 0)
    def _():
        gain_grad_ref[...] = jnp.zeros_like(gain_grad_ref)
        shift_grad_ref[...] = jnp.zeros_like(shift_grad_ref)

    def one(at):
        standard = (x_ref[0, :, at].astype(F32) - center[...]) * inv[...]
        grad = up_ref[0, :, at].astype(F32) + grad_ref[0, :, at].astype(F32)
        product = grad * standard
        gain_grad_ref[:, at] += product
        shift_grad_ref[:, at] += grad
        gain = gain_ref[:, at]
        acc[...] += grad * gain
        acc_cross[...] += product * gain

    each_group(x_ref.shape[2] // span, span, one)
    mean_ref[0] = fold(acc, group, width)
    cross_ref[0] = fold(acc_cross, group, width)


def final_kernel(
    group, width, x_ref, up_ref, grad_ref, center_ref, inv_ref, mean_ref, cross_ref, gain_ref,
    out_ref, center, inv, mean, cross,
):
    span = group * width
    spread(center, center_ref[0], group, width)
    spread(inv, inv_ref[0], group, width)
    spread(mean, mean_ref[0], group, width)
    spread(cross, cross_ref[0], group, width)

    def one(at):
        standard = (x_ref[0, :, at].astype(F32) - center[...]) * inv[...]
        up = up_ref[0, :, at].astype(F32)
        grad = (up + grad_ref[0, :, at].astype(F32)) * gain_ref[:, at]
        out = up + inv[...] * (grad - mean[...] - standard * cross[...])
        out_ref[0, :, at] = out.astype(BF16)

    each_group(x_ref.shape[2] // span, span, one)


def result_kernel(x_ref, normed_ref, filtered_ref, out_ref):
    out = x_ref[...].astype(F32) + normed_ref[...].astype(F32) + filtered_ref[...].astype(F32)
    out_ref[...] = out.astype(BF16)


def row_call(kernel, name, inputs, kinds, out_kinds, sizes, scratch):
    samples, rows_here, lanes, width = sizes
    shapes = {
        "field": (samples, rows_here, lanes),
        "token": (samples, rows_here, width),
        "lane": (1, lanes),
        "sum": (rows_here, lanes),
    }
    specs = {
        "field": pl.BlockSpec((1, rows_here, lanes), lambda b: (b, 0, 0)),
        "token": pl.BlockSpec((1, rows_here, width), lambda b: (b, 0, 0)),
        "lane": pl.BlockSpec((1, lanes), lambda b: (0, 0)),
        "sum": pl.BlockSpec((rows_here, lanes), lambda b: (0, 0)),
    }
    cells = samples * rows_here * lanes
    return pl.pallas_call(
        kernel,
        grid=(samples,),
        in_specs=[specs[kind] for kind in kinds],
        out_specs=[specs[kind] for kind in out_kinds],
        out_shape=[
            jax.ShapeDtypeStruct(shapes[kind], BF16 if kind == "field" else F32)
            for kind in out_kinds
        ],
        scratch_shapes=scratch,
        compiler_params=pltpu.CompilerParams(vmem_limit_bytes=VMEM_BYTES),
        cost_estimate=pl.CostEstimate(
            flops=cells * 2000, bytes_accessed=2 * cells * (len(kinds) + 1), transcendentals=0
        ),
        name=name,
    )(*inputs)


def swap(values):
    return lax.all_to_all(values, "lat", split_axis=0, concat_axis=0, tiled=True)


def channel_sum(first, second, ch):
    both = jnp.stack((first, second))
    if ch == 2:
        both = both + lax.ppermute(both, "ch", [(0, 1), (1, 0)])
    else:
        both = lax.psum(both, "ch")
    return both[0], both[1]


def wide_matrix(matrix):
    high, low = split_table(matrix)
    return jnp.concatenate((high, high, low), axis=2)


def real_matrix(weight):
    turned = jnp.swapaxes(weight, 2, 3)
    top = jnp.concatenate((turned[0], -turned[1]), axis=2)
    bottom = jnp.concatenate((turned[1], turned[0]), axis=2)
    return jnp.concatenate((top, bottom), axis=1)


def weight_grad(grad, block):
    same = grad[:, :block, :block] + grad[:, block:, block:]
    other = grad[:, block:, :block] - grad[:, :block, block:]
    return jnp.swapaxes(jnp.stack((same, other)), 2, 3)


def bias_rows(bias):
    return jnp.concatenate((bias[0], bias[1]), axis=1)[:, :, None]


def bias_grad(grad, block):
    total = jnp.sum(grad, axis=2)
    return jnp.stack((total[:, :block], total[:, block:]))


def body(
    lat, ch, embed, tokens, norm_gain, norm_shift, first_weight, first_bias, second_weight, second_bias, upstream
):
    samples, rows_here, lanes = tokens.shape
    channels = norm_gain.shape[0]
    width = lanes // channels
    height = rows_here * lat
    block = first_weight.shape[2]
    blocks = first_weight.shape[1]
    group = LANE // math.gcd(width, LANE)
    span = group * width
    sizes = (samples, rows_here, lanes, width)
    lat_table = latitude_table(height)
    lon_table, lon_weighted = longitude_table(width)
    lat_forward = left_table(lat_table / math.sqrt(height * width), 2)
    lat_back = left_table(lat_table.T, 1)
    forward_tables = (lat_forward, lat_back, right_table(lon_table, 3), right_table(lon_weighted.T, 1))
    backward_tables = (lat_forward, lat_back, right_table(lon_weighted, 1), right_table(lon_table.T, 1))
    first = real_matrix(first_weight)
    second = real_matrix(second_weight)
    forward_params = (
        wide_matrix(first), bias_rows(first_bias), wide_matrix(second), bias_rows(second_bias),
    )
    backward_params = (
        jnp.swapaxes(first, 1, 2).astype(BF16), jnp.swapaxes(second, 1, 2).astype(BF16),
    )
    gain_lanes = jnp.repeat(norm_gain, width)[None]
    shift_lanes = jnp.repeat(norm_shift, width)[None]
    wide = pltpu.VMEM((rows_here, span), F32)

    early = blocks // 4 * block * width
    upstream_columns = []
    if early:
        upstream_columns.append(swap(upstream[:, :, :early]))
    totals, squares = row_call(
        functools.partial(stats_kernel, group, width), "stats", (tokens,), ("field",),
        ("token", "token"), sizes, [wide, wide],
    )
    totals, squares = channel_sum(totals, squares, ch)
    center = totals / embed
    variance = squares / embed - center * center
    inv_scale = lax.rsqrt(variance + layer_eps)
    (normed,) = row_call(
        functools.partial(norm_kernel, group, width), "norm",
        (tokens, center, inv_scale, gain_lanes, shift_lanes),
        ("field", "token", "token", "lane", "lane"), ("field",), sizes, [wide, wide],
    )
    sent = normed
    if early:
        sent, upstream_columns[0] = lax.optimization_barrier((normed, upstream_columns[0]))
    normed_columns = swap(sent)
    rest, normed_columns = lax.optimization_barrier((upstream[:, :, early:], normed_columns))
    upstream_columns.append(swap(rest))
    filtered, *kept = column_forward(
        normed_columns.reshape(height, lanes), forward_tables, forward_params, group, width, block, 0
    )
    filtered, upstream_columns[-1] = lax.optimization_barrier(
        (filtered.reshape(lat, rows_here, lanes), upstream_columns[-1])
    )
    filtered_rows = swap(filtered)
    spectral, first_grad, first_bias_grad, second_grad, second_bias_grad = column_backward(
        jnp.concatenate(upstream_columns, axis=2).reshape(height, lanes), kept,
        backward_tables, backward_params, group, width, block, 0, 0,
    )
    spectral, filtered_rows = lax.optimization_barrier(
        (spectral.reshape(lat, rows_here, lanes), filtered_rows)
    )
    spectral_rows = swap(spectral)
    (result,) = row_call(
        result_kernel, "result", (tokens, normed, filtered_rows), ("field",) * 3, ("field",), sizes, [],
    )
    first_all = jnp.concatenate(
        (weight_grad(first_grad, block), bias_grad(first_bias_grad, block)[:, :, None]), axis=2
    )
    second_all = jnp.concatenate(
        (weight_grad(second_grad, block), bias_grad(second_bias_grad, block)[:, :, None]), axis=2
    )
    first_all, second_all = lax.psum((first_all, second_all), "lat")
    spectral_rows, result, first_all, second_all = lax.optimization_barrier(
        (spectral_rows, result, first_all, second_all)
    )
    mean, cross, gain_part, shift_part = row_call(
        functools.partial(sums_kernel, group, width), "sums",
        (tokens, upstream, spectral_rows, center, inv_scale, gain_lanes),
        ("field", "field", "field", "token", "token", "lane"),
        ("token", "token", "sum", "sum"), sizes, [wide] * 4,
    )
    gain_part = jnp.sum(gain_part.reshape(rows_here, channels, width), axis=(0, 2))
    shift_part = jnp.sum(shift_part.reshape(rows_here, channels, width), axis=(0, 2))
    mean, cross = channel_sum(mean, cross, ch)
    (grad_tokens,) = row_call(
        functools.partial(final_kernel, group, width), "final",
        (tokens, upstream, spectral_rows, center, inv_scale, mean / embed, cross / embed, gain_lanes),
        ("field", "field", "field", "token", "token", "token", "token", "lane"),
        ("field",), sizes, [wide] * 4,
    )
    vector = jnp.stack((gain_part, shift_part))[None]
    vector = jnp.broadcast_to(vector, (lat, 2, channels))
    gain_grad, shift_grad = jnp.sum(swap(vector), axis=0)
    return (
        result, grad_tokens, first_all[:, :, :block], first_all[:, :, block],
        second_all[:, :, :block], second_all[:, :, block], gain_grad, shift_grad,
    )


def solution(mesh):
    lat = mesh.shape["lat"]
    ch = mesh.shape["ch"]

    def step(tokens, norm_gain, *rest):
        return jax.shard_map(
            functools.partial(body, lat, ch, norm_gain.shape[0]),
            mesh=mesh,
            in_specs=(
                P(None, "lat", "ch"),
                P("ch"),
                P("ch"),
                P(None, "ch", None, None),
                P(None, "ch", None),
                P(None, "ch", None, None),
                P(None, "ch", None),
                P(None, "lat", "ch"),
            ),
            out_specs=(
                P(None, "lat", "ch"),
                P(None, "lat", "ch"),
                P(None, "ch", None, None),
                P(None, "ch", None),
                P(None, "ch", None, None),
                P(None, "ch", None),
                P("ch"),
                P("ch"),
            ),
            check_vma=False,
        )(tokens, norm_gain, *rest)

    return step
```

```python
import functools
import math

import jax
import jax.numpy as jnp
import numpy as np
from jax import lax
from jax.experimental import pallas as pl
from jax.experimental.pallas import tpu as pltpu
from jax.sharding import PartitionSpec as P

layer_eps = 1e-05
shrink_level = 0.1
LANE = 128
PAD = 256
F32 = jnp.float32
BF16 = jnp.bfloat16
GELU_SCALE = math.sqrt(2.0 / math.pi)
GELU_CUBE = 0.044715
VMEM_BYTES = 60 * 1024 * 1024


def split_table(table):
    full = jnp.asarray(table, F32)
    high = lax.reduce_precision(full, 8, 7)
    return high.astype(BF16), (full - high).astype(BF16)


def left_table(table, passes):
    high, low = split_table(table)
    return jnp.concatenate((high, high, low)[:passes] if passes != 2 else (high, low), axis=1)


def right_table(table, passes):
    high, low = split_table(table)
    return jnp.concatenate((high, high, low)[:passes] if passes != 2 else (high, low), axis=0)


def latitude_table(height):
    cells = np.arange(height)
    table = np.zeros((height, height))
    for pair in range(height // 2):
        angle = 2.0 * np.pi * (pair * cells % height) / height
        table[2 * pair] = np.cos(angle)
        table[2 * pair + 1] = -np.sin(angle)
    table[1] = np.cos(np.pi * cells)
    return table


def longitude_table(width):
    modes = width // 2 + 1
    cells = np.arange(width)[:, None]
    angle = 2.0 * np.pi * (cells * np.arange(modes)[None] % width) / width
    table = np.zeros((PAD, PAD))
    table[:width, :modes] = np.cos(angle)
    table[:width, LANE : LANE + modes] = -np.sin(angle)
    doubled = np.full((modes,), 2.0)
    doubled[0] = 1.0
    if width % 2 == 0:
        doubled[-1] = 1.0
    weights = np.zeros((PAD,))
    weights[:modes] = doubled
    weights[LANE : LANE + modes] = doubled
    return table, table * weights[None]


def dot(left, right):
    return jnp.dot(left, right, preferred_element_type=F32)


def dot_rows(left, right):
    return lax.dot_general(left, right, (((1,), (1,)), ((), ())), preferred_element_type=F32)


def pair_forward(values, first, half):
    real_cos = values[:half, :LANE]
    real_sin = values[:half, LANE:]
    imag_cos = values[half:, :LANE]
    imag_sin = values[half:, LANE:]
    re_left = jnp.where(first, real_cos, real_cos - imag_sin)
    re_right = jnp.where(first, imag_cos, real_cos + imag_sin)
    im_left = jnp.where(first, real_sin, imag_cos + real_sin)
    im_right = jnp.where(first, imag_sin, real_sin - imag_cos)
    top = jnp.concatenate((re_left, re_right), axis=1)
    bottom = jnp.concatenate((im_left, im_right), axis=1)
    return jnp.concatenate((top, bottom), axis=0)


def pair_inverse(values, first, half):
    re_left = values[:half, :LANE]
    re_right = values[:half, LANE:]
    im_left = values[half:, :LANE]
    im_right = values[half:, LANE:]
    a = jnp.where(first, re_left, re_left + re_right)
    b = jnp.where(first, im_left, im_left + im_right)
    c = jnp.where(first, re_right, im_left - im_right)
    d = jnp.where(first, im_right, re_right - re_left)
    top = jnp.concatenate((a, b), axis=1)
    bottom = jnp.concatenate((c, d), axis=1)
    return jnp.concatenate((top, bottom), axis=0)


def split(values):
    high = values.astype(BF16)
    return high, (values - high.astype(F32)).astype(BF16)


def to_modes(x_ref, lat_ref, flat, low, high, group, width, block):
    height = x_ref.shape[0]
    span = group * width
    flat[:, span:] = jnp.zeros((height, flat.shape[1] - span), F32)

    def one(step, carry):
        at = pl.multiple_of(step * span, LANE)
        piece = x_ref[:, pl.ds(at, span)]
        if lat_ref.shape[1] == 2 * height:
            piece = jnp.concatenate((piece, piece), axis=0)
        flat[:, :span] = dot(lat_ref[...], piece)
        for channel in range(group):
            start = channel * width
            rows = pl.ds(step * group + channel, height, stride=block)
            low[rows, :] = flat[:, start : start + LANE]
            high[rows, :] = flat[:, start + LANE : start + PAD]
        return carry

    lax.fori_loop(0, block // group, one, 0)


def from_modes(out_ref, lat_ref, flat, low, high, group, width, block):
    height = out_ref.shape[0]
    span = group * width

    def one(step, carry):
        at = pl.multiple_of(step * span, LANE)
        for channel in range(group):
            start = channel * width
            rows = pl.ds(step * group + channel, height, stride=block)
            flat[:, start : start + LANE] = low[rows, :]
            flat[:, start + LANE : start + PAD] = high[rows, :]
        piece = flat[:, :span].astype(BF16)
        out = dot(lat_ref[...], piece) * (1.0 / math.sqrt(height * width))
        out_ref[:, pl.ds(at, span)] = out.astype(BF16)
        return carry

    lax.fori_loop(0, block // group, one, 0)


def load_rows(low, high, rows):
    return jnp.concatenate((low[rows, :], high[rows, :]), axis=1)


def forward_kernel(
    group, width, block, unroll, x_ref, lat_ref, lat_back_ref, lon_ref, lon_back_ref, first_ref,
    first_bias_ref, second_ref, second_bias_ref, out_ref, spec_ref, slope_ref, hidden_ref,
    shrink_ref, flat, low, high,
):
    height = x_ref.shape[0]
    to_modes(x_ref, lat_ref, flat, low, high, group, width, block)
    two = 2 * block

    def one(step, carry):
        rows = pl.ds(pl.multiple_of(step * (unroll * two), 8), unroll * two)
        major, minor = split(load_rows(low, high, rows))
        modes = dot(jnp.concatenate((major, minor, major), axis=1), lon_ref[...])
        backs = []
        for index in range(unroll):
            pair = step * unroll + index
            first = pair == 0
            major, minor = split(pair_forward(modes[index * two : (index + 1) * two], first, block))
            spec_ref[0, pair] = major
            pre = dot(first_ref[0], jnp.concatenate((major, minor, major), axis=0))
            pre = pre + first_bias_ref[0]
            square = pre * pre
            inner = jnp.tanh(GELU_SCALE * (pre + GELU_CUBE * square * pre))
            half = 0.5 * (1.0 + inner)
            slope = half + 0.5 * GELU_SCALE * pre * (1.0 - inner * inner) * (
                1.0 + 3.0 * GELU_CUBE * square
            )
            slope_ref[0, pair] = slope.astype(BF16)
            major, minor = split(pre * half)
            hidden_ref[0, pair] = major
            mixed = dot(second_ref[0], jnp.concatenate((major, minor, major), axis=0))
            mixed = mixed + second_bias_ref[0]
            shrink = jnp.tanh(mixed / shrink_level)
            shrink_ref[0, pair] = (shrink * shrink).astype(BF16)
            mixed = mixed - shrink_level * shrink
            backs.append(pair_inverse(mixed, first, block).astype(BF16))
        back = dot(jnp.concatenate(backs, axis=0), lon_back_ref[...])
        low[rows, :] = back[:, :LANE]
        high[rows, :] = back[:, LANE:]
        return carry

    lax.fori_loop(0, height // (2 * unroll), one, 0)
    from_modes(out_ref, lat_back_ref, flat, low, high, group, width, block)


def backward_kernel(
    group, width, block, unroll, x_ref, spec_ref, slope_ref, hidden_ref, shrink_ref, lat_ref,
    lat_back_ref, lon_ref, lon_back_ref, first_ref, second_ref, out_ref, first_grad_ref,
    first_bias_grad_ref, second_grad_ref, second_bias_grad_ref, flat, low, high,
):
    height = x_ref.shape[0]
    to_modes(x_ref, lat_ref, flat, low, high, group, width, block)
    two = 2 * block
    first_grad_ref[...] = jnp.zeros_like(first_grad_ref)
    second_grad_ref[...] = jnp.zeros_like(second_grad_ref)
    first_bias_grad_ref[...] = jnp.zeros_like(first_bias_grad_ref)
    second_bias_grad_ref[...] = jnp.zeros_like(second_bias_grad_ref)

    def one(step, carry):
        rows = pl.ds(pl.multiple_of(step * (unroll * two), 8), unroll * two)
        modes = dot(load_rows(low, high, rows).astype(BF16), lon_ref[...])
        backs = []
        grads = []
        for index in range(unroll):
            pair = step * unroll + index
            first = pair == 0
            grad = pair_forward(modes[index * two : (index + 1) * two], first, block)
            outer = grad * shrink_ref[0, pair].astype(F32)
            outer_low = outer.astype(BF16)
            inner = dot(second_ref[0], outer_low) * slope_ref[0, pair].astype(F32)
            inner_low = inner.astype(BF16)
            back = pair_inverse(dot(first_ref[0], inner_low), first, block)
            backs.append(back.astype(BF16))
            grads.append((outer, outer_low, inner, inner_low))
        hiddens = jnp.concatenate([hidden_ref[0, step * unroll + i] for i in range(unroll)], axis=1)
        specs = jnp.concatenate([spec_ref[0, step * unroll + i] for i in range(unroll)], axis=1)
        outers = jnp.concatenate([grad[1] for grad in grads], axis=1)
        inners = jnp.concatenate([grad[3] for grad in grads], axis=1)
        second_grad_ref[0] += dot_rows(outers, hiddens)
        first_grad_ref[0] += dot_rows(inners, specs)
        outer_sum = sum(grad[0][:, :LANE] + grad[0][:, LANE:] for grad in grads)
        inner_sum = sum(grad[2][:, :LANE] + grad[2][:, LANE:] for grad in grads)
        second_bias_grad_ref[0] += outer_sum
        first_bias_grad_ref[0] += inner_sum
        back = dot(jnp.concatenate(backs, axis=0), lon_back_ref[...])
        low[rows, :] = back[:, :LANE]
        high[rows, :] = back[:, LANE:]
        return carry

    lax.fori_loop(0, height // (2 * unroll), one, 0)
    from_modes(out_ref, lat_back_ref, flat, low, high, group, width, block)


def whole(array):
    rank = array.ndim
    return pl.BlockSpec(array.shape, lambda *_: (0,) * rank)


def per_block(shape, offset=0):
    rank = len(shape)
    return pl.BlockSpec((1,) + tuple(shape), lambda n: (n + offset,) + (0,) * rank)


def column_scratch(height, group, width, block):
    return [
        pltpu.VMEM((height, group * width + LANE), F32),
        pltpu.VMEM((height * block, LANE), F32),
        pltpu.VMEM((height * block, LANE), F32),
    ]


def column_forward(x, tables, params, group, width, block, start, unroll=4):
    height, lanes = x.shape
    blocks = lanes // (block * width)
    pairs = height // 2
    two = 2 * block
    wide = pl.BlockSpec((height, block * width), lambda n: (0, n))
    kept = per_block((pairs, two, PAD))
    cells = blocks * pairs * two * PAD
    return pl.pallas_call(
        functools.partial(forward_kernel, group, width, block, unroll),
        grid=(blocks,),
        in_specs=[
            wide, *[whole(table) for table in tables],
            per_block((two, 3 * two), start), per_block((two, 1), start),
            per_block((two, 3 * two), start), per_block((two, 1), start),
        ],
        out_specs=[wide] + [kept] * 4,
        out_shape=[jax.ShapeDtypeStruct(x.shape, BF16)]
        + [jax.ShapeDtypeStruct((blocks, pairs, two, PAD), BF16)] * 4,
        scratch_shapes=column_scratch(height, group, width, block),
        compiler_params=pltpu.CompilerParams(vmem_limit_bytes=VMEM_BYTES),
        cost_estimate=pl.CostEstimate(
            flops=cells * 4000, bytes_accessed=4 * height * lanes + 8 * cells, transcendentals=0
        ),
        name="column_forward",
    )(x, *tables, *params)


def column_backward(x, kept_arrays, tables, params, group, width, block, start, local, unroll=4):
    height, lanes = x.shape
    blocks = lanes // (block * width)
    pairs = height // 2
    two = 2 * block
    wide = pl.BlockSpec((height, block * width), lambda n: (0, n))
    kept = per_block((pairs, two, PAD), local)
    cells = blocks * pairs * two * PAD
    sizes = ((two, two), (two, LANE)) * 2
    return pl.pallas_call(
        functools.partial(backward_kernel, group, width, block, unroll),
        grid=(blocks,),
        in_specs=[
            wide, kept, kept, kept, kept, *[whole(table) for table in tables],
            per_block((two, two), start), per_block((two, two), start),
        ],
        out_specs=[wide] + [per_block(size) for size in sizes],
        out_shape=[jax.ShapeDtypeStruct(x.shape, BF16)]
        + [jax.ShapeDtypeStruct((blocks,) + size, F32) for size in sizes],
        scratch_shapes=column_scratch(height, group, width, block),
        compiler_params=pltpu.CompilerParams(vmem_limit_bytes=VMEM_BYTES),
        cost_estimate=pl.CostEstimate(
            flops=cells * 4000, bytes_accessed=4 * height * lanes + 8 * cells, transcendentals=0
        ),
        name="column_backward",
    )(x, *kept_arrays, *tables, *params)


def fold(acc, group, width):
    total = acc[:, :width]
    for channel in range(1, group):
        total = total + acc[:, channel * width : (channel + 1) * width]
    return total


def spread(wide, token, group, width):
    for channel in range(group):
        wide[:, channel * width : (channel + 1) * width] = token


def each_group(groups, span, step_body):
    def one(step, carry):
        step_body(pl.ds(pl.multiple_of(step * span, LANE), span))
        return carry

    lax.fori_loop(0, groups, one, 0)


def stats_kernel(group, width, x_ref, total_ref, square_ref, acc, acc_square):
    span = group * width
    acc[...] = jnp.zeros_like(acc)
    acc_square[...] = jnp.zeros_like(acc_square)

    def one(at):
        piece = x_ref[0, :, at].astype(F32)
        acc[...] += piece
        acc_square[...] += piece * piece

    each_group(x_ref.shape[2] // span, span, one)
    total_ref[0] = fold(acc, group, width)
    square_ref[0] = fold(acc_square, group, width)


def norm_kernel(group, width, x_ref, center_ref, inv_ref, gain_ref, shift_ref, out_ref, center, inv):
    span = group * width
    spread(center, center_ref[0], group, width)
    spread(inv, inv_ref[0], group, width)

    def one(at):
        standard = (x_ref[0, :, at].astype(F32) - center[...]) * inv[...]
        out_ref[0, :, at] = (standard * gain_ref[:, at] + shift_ref[:, at]).astype(BF16)

    each_group(x_ref.shape[2] // span, span, one)


def spread_token(wide, ring, token, halves, width):
    token = jnp.concatenate((token,) * halves, axis=0)
    ring[:, :width] = token
    ring[:, width : 2 * width] = token
    for tile in range(wide.shape[1] // LANE):
        start = tile * LANE % width
        wide[:, tile * LANE : (tile + 1) * LANE] = ring[:, start : start + LANE]


def fold_halves(acc, group, width, halves):
    total = fold(acc, group, width)
    rows = total.shape[0] // halves
    return sum(total[half * rows : (half + 1) * rows] for half in range(halves))


def each_chunk(span, chunk_body):
    chunk = span // math.gcd(span // LANE, 9)

    def one(step, carry):
        chunk_body(pl.multiple_of(step * chunk, LANE), chunk)
        return carry

    lax.fori_loop(0, span // chunk, one, 0)


def sums_kernel(
    group, width, halves, x_ref, up_ref, grad_ref, inv_ref, offset_ref, gain_ref,
    mean_ref, cross_ref, gain_grad_ref, shift_grad_ref, ring, inv, offset, acc, acc_cross,
):
    span = group * width
    groups = x_ref.shape[2] // span
    spread_token(inv, ring, inv_ref[0], halves, width)
    spread_token(offset, ring, offset_ref[0], halves, width)

    @pl.when(pl.program_id(0) == 0)
    def _():
        gain_grad_ref[...] = jnp.zeros_like(gain_grad_ref)
        shift_grad_ref[...] = jnp.zeros_like(shift_grad_ref)

    def one(start, chunk):
        here = pl.ds(start, chunk)
        inv_here = inv[:, here]
        offset_here = offset[:, here]
        mean = jnp.zeros((inv.shape[0], chunk), F32)
        cross = jnp.zeros((inv.shape[0], chunk), F32)
        for step in range(groups):
            at = pl.ds(pl.multiple_of(start + step * span, LANE), chunk)
            standard = x_ref[0, :, at].astype(F32) * inv_here - offset_here
            grad = up_ref[0, :, at].astype(F32) + grad_ref[0, :, at].astype(F32)
            gain_grad_ref[:, at] += grad * standard
            shift_grad_ref[:, at] += grad
            grad = grad * gain_ref[:, at]
            mean = mean + grad
            cross = cross + grad * standard
        acc[:, here] = mean
        acc_cross[:, here] = cross

    each_chunk(span, one)
    mean_ref[0] = fold_halves(acc, group, width, halves)
    cross_ref[0] = fold_halves(acc_cross, group, width, halves)


def final_kernel(
    group, width, halves, x_ref, up_ref, grad_ref, inv_ref, slope_ref, level_ref, gain_ref,
    out_ref, ring, inv, slope, level,
):
    span = group * width
    lanes = x_ref.shape[2]
    rows = out_ref.shape[1]
    spread_token(inv, ring, inv_ref[0], halves, width)
    spread_token(slope, ring, slope_ref[0], halves, width)
    spread_token(level, ring, level_ref[0], halves, width)

    def one(start, chunk):
        here = pl.ds(start, chunk)
        inv_here = inv[:, here]
        slope_here = slope[:, here]
        level_here = level[:, here]
        for step in range(lanes // span):
            place = start + step * span
            at = pl.ds(pl.multiple_of(place, LANE), chunk)
            up = up_ref[0, :, at].astype(F32)
            grad = (up + grad_ref[0, :, at].astype(F32)) * gain_ref[:, at]
            out = up + inv_here * grad + (level_here - x_ref[0, :, at].astype(F32) * slope_here)
            for half in range(halves):
                there = pl.ds(pl.multiple_of(place + half * lanes, LANE), chunk)
                out_ref[0, :, there] = out[half * rows : (half + 1) * rows].astype(BF16)

    each_chunk(span, one)


def result_kernel(x_ref, normed_ref, filtered_ref, out_ref):
    out = x_ref[...].astype(F32) + normed_ref[...].astype(F32) + filtered_ref[...].astype(F32)
    out_ref[...] = out.astype(BF16)


def row_call(kernel, name, inputs, kinds, out_kinds, sizes, scratch):
    samples, rows_here, lanes, width, halves = sizes
    many = halves * rows_here
    part = lanes // halves
    shapes = {
        "packed": (samples, many, part),
        "packed_lane": (many, part),
        "field": (samples, rows_here, lanes),
        "token": (samples, rows_here, width),
        "lane": (1, lanes),
        "sum": (many, part),
    }
    specs = {
        "packed": pl.BlockSpec((1, many, part), lambda b: (b, 0, 0)),
        "packed_lane": pl.BlockSpec((many, part), lambda b: (0, 0)),
        "field": pl.BlockSpec((1, rows_here, lanes), lambda b: (b, 0, 0)),
        "token": pl.BlockSpec((1, rows_here, width), lambda b: (b, 0, 0)),
        "lane": pl.BlockSpec((1, lanes), lambda b: (0, 0)),
        "sum": pl.BlockSpec((many, part), lambda b: (0, 0)),
    }
    cells = samples * rows_here * lanes
    return pl.pallas_call(
        kernel,
        grid=(samples,),
        in_specs=[specs[kind] for kind in kinds],
        out_specs=[specs[kind] for kind in out_kinds],
        out_shape=[
            jax.ShapeDtypeStruct(shapes[kind], BF16 if kind == "field" else F32)
            for kind in out_kinds
        ],
        scratch_shapes=scratch,
        compiler_params=pltpu.CompilerParams(vmem_limit_bytes=VMEM_BYTES),
        cost_estimate=pl.CostEstimate(
            flops=cells * 2000, bytes_accessed=2 * cells * (len(kinds) + 1), transcendentals=0
        ),
        name=name,
    )(*inputs)


def swap(values):
    return lax.all_to_all(values, "lat", split_axis=0, concat_axis=0, tiled=True)


def channel_sum(first, second, ch):
    both = jnp.stack((first, second))
    if ch == 2:
        both = both + lax.ppermute(both, "ch", [(0, 1), (1, 0)])
    else:
        both = lax.psum(both, "ch")
    return both[0], both[1]


def wide_matrix(matrix):
    high, low = split_table(matrix)
    return jnp.concatenate((high, high, low), axis=2)


def real_matrix(weight):
    turned = jnp.swapaxes(weight, 2, 3)
    top = jnp.concatenate((turned[0], -turned[1]), axis=2)
    bottom = jnp.concatenate((turned[1], turned[0]), axis=2)
    return jnp.concatenate((top, bottom), axis=1)


def weight_grad(grad, block):
    same = grad[:, :block, :block] + grad[:, block:, block:]
    other = grad[:, block:, :block] - grad[:, :block, block:]
    return jnp.swapaxes(jnp.stack((same, other)), 2, 3)


def bias_rows(bias):
    return jnp.concatenate((bias[0], bias[1]), axis=1)[:, :, None]


def bias_grad(grad, block):
    total = jnp.sum(grad, axis=2)
    return jnp.stack((total[:, :block], total[:, block:]))


def body(
    lat, ch, embed, tokens, norm_gain, norm_shift, first_weight, first_bias, second_weight, second_bias, upstream
):
    samples, rows_here, lanes = tokens.shape
    channels = norm_gain.shape[0]
    width = lanes // channels
    height = rows_here * lat
    block = first_weight.shape[2]
    blocks = first_weight.shape[1]
    group = LANE // math.gcd(width, LANE)
    span = group * width
    halves = 2 if channels % (2 * group) == 0 else 1
    many = halves * rows_here
    part = lanes // halves
    sizes = (samples, rows_here, lanes, width, halves)

    def pack(values):
        pieces = [values[..., half * part : (half + 1) * part] for half in range(halves)]
        return jnp.concatenate(
            [piece.reshape(samples, rows_here, part) for piece in pieces], axis=1
        )

    lat_table = latitude_table(height)
    lon_table, lon_weighted = longitude_table(width)
    lat_forward = left_table(lat_table / math.sqrt(height * width), 2)
    lat_back = left_table(lat_table.T, 1)
    forward_tables = (lat_forward, lat_back, right_table(lon_table, 3), right_table(lon_weighted.T, 1))
    backward_tables = (lat_forward, lat_back, right_table(lon_weighted, 1), right_table(lon_table.T, 1))
    first = real_matrix(first_weight)
    second = real_matrix(second_weight)
    forward_params = (
        wide_matrix(first), bias_rows(first_bias), wide_matrix(second), bias_rows(second_bias),
    )
    backward_params = (
        jnp.swapaxes(first, 1, 2).astype(BF16), jnp.swapaxes(second, 1, 2).astype(BF16),
    )
    gain_lanes = jnp.repeat(norm_gain, width)[None]
    shift_lanes = jnp.repeat(norm_shift, width)[None]
    wide = pltpu.VMEM((rows_here, span), F32)

    early = blocks // 4 * block * width
    upstream_columns = []
    if early:
        upstream_columns.append(swap(upstream[:, :, :early]))
    totals, squares = row_call(
        functools.partial(stats_kernel, group, width), "stats", (tokens,), ("field",),
        ("token", "token"), sizes, [wide, wide],
    )
    totals, squares = channel_sum(totals, squares, ch)
    center = totals / embed
    variance = squares / embed - center * center
    inv_scale = lax.rsqrt(variance + layer_eps)
    (normed,) = row_call(
        functools.partial(norm_kernel, group, width), "norm",
        (tokens, center, inv_scale, gain_lanes, shift_lanes),
        ("field", "token", "token", "lane", "lane"), ("field",), sizes, [wide, wide],
    )
    sent = normed
    if early:
        sent, upstream_columns[0] = lax.optimization_barrier((normed, upstream_columns[0]))
    normed_columns = swap(sent)
    gain_packed = jnp.broadcast_to(
        gain_lanes.reshape(halves, 1, part), (halves, rows_here, part)
    ).reshape(many, part)
    rest, normed_columns, forward_params, backward_params, packs = lax.optimization_barrier(
        (
            upstream[:, :, early:], normed_columns, forward_params, backward_params,
            (pack(tokens), pack(upstream), gain_packed, center * inv_scale),
        )
    )
    tokens_packed, upstream_packed, gain_packed, offset = packs
    upstream_columns.append(swap(rest))
    filtered, *kept = column_forward(
        normed_columns.reshape(height, lanes), forward_tables, forward_params, group, width, block, 0
    )
    filtered, upstream_columns[-1] = lax.optimization_barrier(
        (filtered.reshape(lat, rows_here, lanes), upstream_columns[-1])
    )
    filtered_rows = swap(filtered)
    spectral, first_grad, first_bias_grad, second_grad, second_bias_grad = column_backward(
        jnp.concatenate(upstream_columns, axis=2).reshape(height, lanes), kept,
        backward_tables, backward_params, group, width, block, 0, 0,
    )
    first_all = jnp.concatenate(
        (weight_grad(first_grad, block), bias_grad(first_bias_grad, block)[:, :, None]), axis=2
    )
    second_all = jnp.concatenate(
        (weight_grad(second_grad, block), bias_grad(second_bias_grad, block)[:, :, None]), axis=2
    )
    spectral, filtered_rows, first_all, second_all = lax.optimization_barrier(
        (pack(spectral), filtered_rows, first_all, second_all)
    )
    spectral_rows = swap(spectral)
    (result,) = row_call(
        result_kernel, "result", (tokens, normed, filtered_rows), ("field",) * 3, ("field",), sizes, [],
    )
    first_all, second_all = lax.psum((first_all, second_all), "lat")
    spectral_rows, result = lax.optimization_barrier((spectral_rows, result))
    wide = pltpu.VMEM((many, span), F32)
    ring = pltpu.VMEM((many, 2 * width + LANE), F32)
    mean, cross, gain_part, shift_part = row_call(
        functools.partial(sums_kernel, group, width, halves), "sums",
        (tokens_packed, upstream_packed, spectral_rows, inv_scale, offset, gain_packed),
        ("packed", "packed", "packed", "token", "token", "packed_lane"),
        ("token", "token", "sum", "sum"), sizes, [ring] + [wide] * 4,
    )
    mean, cross = channel_sum(mean, cross, ch)
    mean, first_all, second_all = lax.optimization_barrier((mean, first_all, second_all))
    cross = cross * inv_scale / embed
    (grad_tokens,) = row_call(
        functools.partial(final_kernel, group, width, halves), "final",
        (
            tokens_packed, upstream_packed, spectral_rows, inv_scale, cross * inv_scale,
            cross * offset - mean * inv_scale / embed, gain_packed,
        ),
        ("packed", "packed", "packed", "token", "token", "token", "packed_lane"),
        ("field",), sizes, [ring] + [wide] * 3,
    )
    parts = jnp.stack((gain_part, shift_part)).reshape(2, halves, rows_here, channels // halves, width)
    vector = jnp.broadcast_to(jnp.sum(parts, axis=(2, 4)).reshape(1, 2, channels), (lat, 2, channels))
    gathered = swap(vector)
    gathered, grad_tokens = lax.optimization_barrier((gathered, grad_tokens))
    gain_grad, shift_grad = jnp.sum(gathered, axis=0)
    return (
        result, grad_tokens, first_all[:, :, :block], first_all[:, :, block],
        second_all[:, :, :block], second_all[:, :, block], gain_grad, shift_grad,
    )


def solution(mesh):
    lat = mesh.shape["lat"]
    ch = mesh.shape["ch"]

    def step(tokens, norm_gain, *rest):
        return jax.shard_map(
            functools.partial(body, lat, ch, norm_gain.shape[0]),
            mesh=mesh,
            in_specs=(
                P(None, "lat", "ch"),
                P("ch"),
                P("ch"),
                P(None, "ch", None, None),
                P(None, "ch", None),
                P(None, "ch", None, None),
                P(None, "ch", None),
                P(None, "lat", "ch"),
            ),
            out_specs=(
                P(None, "lat", "ch"),
                P(None, "lat", "ch"),
                P(None, "ch", None, None),
                P(None, "ch", None),
                P(None, "ch", None, None),
                P(None, "ch", None),
                P("ch"),
                P("ch"),
            ),
            check_vma=False,
        )(tokens, norm_gain, *rest)

    return step
```

```python
import functools
import math

import jax
import jax.numpy as jnp
import numpy as np
from jax import lax
from jax.experimental import pallas as pl
from jax.experimental.pallas import tpu as pltpu
from jax.sharding import PartitionSpec as P

layer_eps = 1e-05
shrink_level = 0.1
LANE = 128
PAD = 256
F32 = jnp.float32
BF16 = jnp.bfloat16
GELU_SCALE = math.sqrt(2.0 / math.pi)
GELU_CUBE = 0.044715
VMEM_BYTES = 60 * 1024 * 1024


def split_table(table):
    full = jnp.asarray(table, F32)
    high = lax.reduce_precision(full, 8, 7)
    return high.astype(BF16), (full - high).astype(BF16)


def left_table(table, passes):
    high, low = split_table(table)
    return jnp.concatenate((high, high, low)[:passes] if passes != 2 else (high, low), axis=1)


def right_table(table, passes):
    high, low = split_table(table)
    return jnp.concatenate((high, high, low)[:passes] if passes != 2 else (high, low), axis=0)


def latitude_table(height):
    cells = np.arange(height)
    table = np.zeros((height, height))
    for pair in range(height // 2):
        angle = 2.0 * np.pi * (pair * cells % height) / height
        table[2 * pair] = np.cos(angle)
        table[2 * pair + 1] = -np.sin(angle)
    table[1] = np.cos(np.pi * cells)
    return table


def longitude_table(width):
    modes = width // 2 + 1
    cells = np.arange(width)[:, None]
    angle = 2.0 * np.pi * (cells * np.arange(modes)[None] % width) / width
    table = np.zeros((PAD, PAD))
    table[:width, :modes] = np.cos(angle)
    table[:width, LANE : LANE + modes] = -np.sin(angle)
    doubled = np.full((modes,), 2.0)
    doubled[0] = 1.0
    if width % 2 == 0:
        doubled[-1] = 1.0
    weights = np.zeros((PAD,))
    weights[:modes] = doubled
    weights[LANE : LANE + modes] = doubled
    return table, table * weights[None]


def dot(left, right):
    return jnp.dot(left, right, preferred_element_type=F32)


def dot_rows(left, right):
    return lax.dot_general(left, right, (((1,), (1,)), ((), ())), preferred_element_type=F32)


def pair_forward(values, first, half):
    real_cos = values[:half, :LANE]
    real_sin = values[:half, LANE:]
    imag_cos = values[half:, :LANE]
    imag_sin = values[half:, LANE:]
    re_left = jnp.where(first, real_cos, real_cos - imag_sin)
    re_right = jnp.where(first, imag_cos, real_cos + imag_sin)
    im_left = jnp.where(first, real_sin, imag_cos + real_sin)
    im_right = jnp.where(first, imag_sin, real_sin - imag_cos)
    top = jnp.concatenate((re_left, re_right), axis=1)
    bottom = jnp.concatenate((im_left, im_right), axis=1)
    return jnp.concatenate((top, bottom), axis=0)


def pair_inverse(values, first, half):
    re_left = values[:half, :LANE]
    re_right = values[:half, LANE:]
    im_left = values[half:, :LANE]
    im_right = values[half:, LANE:]
    a = jnp.where(first, re_left, re_left + re_right)
    b = jnp.where(first, im_left, im_left + im_right)
    c = jnp.where(first, re_right, im_left - im_right)
    d = jnp.where(first, im_right, re_right - re_left)
    top = jnp.concatenate((a, b), axis=1)
    bottom = jnp.concatenate((c, d), axis=1)
    return jnp.concatenate((top, bottom), axis=0)


def split(values):
    high = values.astype(BF16)
    return high, (values - high.astype(F32)).astype(BF16)


def to_modes(x_ref, lat_ref, flat, low, high, group, width, block):
    height = x_ref.shape[0]
    span = group * width
    flat[:, span:] = jnp.zeros((height, flat.shape[1] - span), F32)

    def one(step, carry):
        at = pl.multiple_of(step * span, LANE)
        piece = x_ref[:, pl.ds(at, span)]
        if lat_ref.shape[1] == 2 * height:
            piece = jnp.concatenate((piece, piece), axis=0)
        flat[:, :span] = dot(lat_ref[...], piece)
        for channel in range(group):
            start = channel * width
            rows = pl.ds(step * group + channel, height, stride=block)
            low[rows, :] = flat[:, start : start + LANE]
            high[rows, :] = flat[:, start + LANE : start + PAD]
        return carry

    lax.fori_loop(0, block // group, one, 0)


def from_modes(out_ref, lat_ref, flat, low, high, group, width, block):
    height = out_ref.shape[0]
    span = group * width

    def one(step, carry):
        at = pl.multiple_of(step * span, LANE)
        for channel in range(group):
            start = channel * width
            rows = pl.ds(step * group + channel, height, stride=block)
            flat[:, start : start + LANE] = low[rows, :]
            flat[:, start + LANE : start + PAD] = high[rows, :]
        piece = flat[:, :span].astype(BF16)
        out = dot(lat_ref[...], piece) * (1.0 / math.sqrt(height * width))
        out_ref[:, pl.ds(at, span)] = out.astype(BF16)
        return carry

    lax.fori_loop(0, block // group, one, 0)


def load_rows(low, high, rows):
    return jnp.concatenate((low[rows, :], high[rows, :]), axis=1)


def forward_kernel(
    group, width, block, unroll, x_ref, lat_ref, lat_back_ref, lon_ref, lon_back_ref, first_ref,
    first_bias_ref, second_ref, second_bias_ref, out_ref, spec_ref, slope_ref, hidden_ref,
    shrink_ref, flat, low, high,
):
    height = x_ref.shape[0]
    to_modes(x_ref, lat_ref, flat, low, high, group, width, block)
    two = 2 * block

    def one(step, carry):
        rows = pl.ds(pl.multiple_of(step * (unroll * two), 8), unroll * two)
        major, minor = split(load_rows(low, high, rows))
        modes = dot(jnp.concatenate((major, minor, major), axis=1), lon_ref[...])
        backs = []
        for index in range(unroll):
            pair = step * unroll + index
            first = pair == 0
            major, minor = split(pair_forward(modes[index * two : (index + 1) * two], first, block))
            spec_ref[0, pair] = major
            pre = dot(first_ref[0], jnp.concatenate((major, minor, major), axis=0))
            pre = pre + first_bias_ref[0]
            square = pre * pre
            inner = jnp.tanh(GELU_SCALE * (pre + GELU_CUBE * square * pre))
            half = 0.5 * (1.0 + inner)
            slope = half + 0.5 * GELU_SCALE * pre * (1.0 - inner * inner) * (
                1.0 + 3.0 * GELU_CUBE * square
            )
            slope_ref[0, pair] = slope.astype(BF16)
            major, minor = split(pre * half)
            hidden_ref[0, pair] = major
            mixed = dot(second_ref[0], jnp.concatenate((major, minor, major), axis=0))
            mixed = mixed + second_bias_ref[0]
            shrink = jnp.tanh(mixed / shrink_level)
            shrink_ref[0, pair] = (shrink * shrink).astype(BF16)
            mixed = mixed - shrink_level * shrink
            backs.append(pair_inverse(mixed, first, block).astype(BF16))
        back = dot(jnp.concatenate(backs, axis=0), lon_back_ref[...])
        low[rows, :] = back[:, :LANE]
        high[rows, :] = back[:, LANE:]
        return carry

    lax.fori_loop(0, height // (2 * unroll), one, 0)
    from_modes(out_ref, lat_back_ref, flat, low, high, group, width, block)


def backward_kernel(
    group, width, block, unroll, x_ref, spec_ref, slope_ref, hidden_ref, shrink_ref, lat_ref,
    lat_back_ref, lon_ref, lon_back_ref, first_ref, second_ref, out_ref, first_grad_ref,
    first_bias_grad_ref, second_grad_ref, second_bias_grad_ref, flat, low, high,
):
    height = x_ref.shape[0]
    to_modes(x_ref, lat_ref, flat, low, high, group, width, block)
    two = 2 * block
    first_grad_ref[...] = jnp.zeros_like(first_grad_ref)
    second_grad_ref[...] = jnp.zeros_like(second_grad_ref)
    first_bias_grad_ref[...] = jnp.zeros_like(first_bias_grad_ref)
    second_bias_grad_ref[...] = jnp.zeros_like(second_bias_grad_ref)

    def one(step, carry):
        rows = pl.ds(pl.multiple_of(step * (unroll * two), 8), unroll * two)
        modes = dot(load_rows(low, high, rows).astype(BF16), lon_ref[...])
        backs = []
        grads = []
        for index in range(unroll):
            pair = step * unroll + index
            first = pair == 0
            grad = pair_forward(modes[index * two : (index + 1) * two], first, block)
            outer = grad * shrink_ref[0, pair].astype(F32)
            outer_low = outer.astype(BF16)
            inner = dot(second_ref[0], outer_low) * slope_ref[0, pair].astype(F32)
            inner_low = inner.astype(BF16)
            back = pair_inverse(dot(first_ref[0], inner_low), first, block)
            backs.append(back.astype(BF16))
            grads.append((outer, outer_low, inner, inner_low))
        hiddens = jnp.concatenate([hidden_ref[0, step * unroll + i] for i in range(unroll)], axis=1)
        specs = jnp.concatenate([spec_ref[0, step * unroll + i] for i in range(unroll)], axis=1)
        outers = jnp.concatenate([grad[1] for grad in grads], axis=1)
        inners = jnp.concatenate([grad[3] for grad in grads], axis=1)
        second_grad_ref[0] += dot_rows(outers, hiddens)
        first_grad_ref[0] += dot_rows(inners, specs)
        outer_sum = sum(grad[0][:, :LANE] + grad[0][:, LANE:] for grad in grads)
        inner_sum = sum(grad[2][:, :LANE] + grad[2][:, LANE:] for grad in grads)
        second_bias_grad_ref[0] += outer_sum
        first_bias_grad_ref[0] += inner_sum
        back = dot(jnp.concatenate(backs, axis=0), lon_back_ref[...])
        low[rows, :] = back[:, :LANE]
        high[rows, :] = back[:, LANE:]
        return carry

    lax.fori_loop(0, height // (2 * unroll), one, 0)
    from_modes(out_ref, lat_back_ref, flat, low, high, group, width, block)


def whole(array):
    rank = array.ndim
    return pl.BlockSpec(array.shape, lambda *_: (0,) * rank)


def per_block(shape, offset=0):
    rank = len(shape)
    return pl.BlockSpec((1,) + tuple(shape), lambda n: (n + offset,) + (0,) * rank)


def column_scratch(height, group, width, block):
    return [
        pltpu.VMEM((height, group * width + LANE), F32),
        pltpu.VMEM((height * block, LANE), F32),
        pltpu.VMEM((height * block, LANE), F32),
    ]


def column_forward(x, tables, params, group, width, block, start, unroll=4):
    height, lanes = x.shape
    blocks = lanes // (block * width)
    pairs = height // 2
    two = 2 * block
    wide = pl.BlockSpec((height, block * width), lambda n: (0, n))
    kept = per_block((pairs, two, PAD))
    cells = blocks * pairs * two * PAD
    return pl.pallas_call(
        functools.partial(forward_kernel, group, width, block, unroll),
        grid=(blocks,),
        in_specs=[
            wide, *[whole(table) for table in tables],
            per_block((two, 3 * two), start), per_block((two, 1), start),
            per_block((two, 3 * two), start), per_block((two, 1), start),
        ],
        out_specs=[wide] + [kept] * 4,
        out_shape=[jax.ShapeDtypeStruct(x.shape, BF16)]
        + [jax.ShapeDtypeStruct((blocks, pairs, two, PAD), BF16)] * 4,
        scratch_shapes=column_scratch(height, group, width, block),
        compiler_params=pltpu.CompilerParams(vmem_limit_bytes=VMEM_BYTES),
        cost_estimate=pl.CostEstimate(
            flops=cells * 4000, bytes_accessed=4 * height * lanes + 8 * cells, transcendentals=0
        ),
        name="column_forward",
    )(x, *tables, *params)


def column_backward(x, kept_arrays, tables, params, group, width, block, start, local, unroll=4):
    height, lanes = x.shape
    blocks = lanes // (block * width)
    pairs = height // 2
    two = 2 * block
    wide = pl.BlockSpec((height, block * width), lambda n: (0, n))
    kept = per_block((pairs, two, PAD), local)
    cells = blocks * pairs * two * PAD
    sizes = ((two, two), (two, LANE)) * 2
    return pl.pallas_call(
        functools.partial(backward_kernel, group, width, block, unroll),
        grid=(blocks,),
        in_specs=[
            wide, kept, kept, kept, kept, *[whole(table) for table in tables],
            per_block((two, two), start), per_block((two, two), start),
        ],
        out_specs=[wide] + [per_block(size) for size in sizes],
        out_shape=[jax.ShapeDtypeStruct(x.shape, BF16)]
        + [jax.ShapeDtypeStruct((blocks,) + size, F32) for size in sizes],
        scratch_shapes=column_scratch(height, group, width, block),
        compiler_params=pltpu.CompilerParams(vmem_limit_bytes=VMEM_BYTES),
        cost_estimate=pl.CostEstimate(
            flops=cells * 4000, bytes_accessed=4 * height * lanes + 8 * cells, transcendentals=0
        ),
        name="column_backward",
    )(x, *kept_arrays, *tables, *params)


def fold(acc, group, width):
    total = acc[:, :width]
    for channel in range(1, group):
        total = total + acc[:, channel * width : (channel + 1) * width]
    return total


def spread(wide, token, group, width):
    for channel in range(group):
        wide[:, channel * width : (channel + 1) * width] = token


def each_group(groups, span, step_body):
    def one(step, carry):
        step_body(pl.ds(pl.multiple_of(step * span, LANE), span))
        return carry

    lax.fori_loop(0, groups, one, 0)


def stats_kernel(group, width, x_ref, total_ref, square_ref, acc, acc_square):
    span = group * width
    acc[...] = jnp.zeros_like(acc)
    acc_square[...] = jnp.zeros_like(acc_square)

    def one(at):
        piece = x_ref[0, :, at].astype(F32)
        acc[...] += piece
        acc_square[...] += piece * piece

    each_group(x_ref.shape[2] // span, span, one)
    total_ref[0] = fold(acc, group, width)
    square_ref[0] = fold(acc_square, group, width)


def norm_kernel(group, width, x_ref, center_ref, inv_ref, gain_ref, shift_ref, out_ref, center, inv):
    span = group * width
    spread(center, center_ref[0], group, width)
    spread(inv, inv_ref[0], group, width)

    def one(at):
        standard = (x_ref[0, :, at].astype(F32) - center[...]) * inv[...]
        out_ref[0, :, at] = (standard * gain_ref[:, at] + shift_ref[:, at]).astype(BF16)

    each_group(x_ref.shape[2] // span, span, one)


def spread_token(wide, ring, token, halves, width):
    token = jnp.concatenate((token,) * halves, axis=0)
    ring[:, :width] = token
    ring[:, width : 2 * width] = token
    for tile in range(wide.shape[1] // LANE):
        start = tile * LANE % width
        wide[:, tile * LANE : (tile + 1) * LANE] = ring[:, start : start + LANE]


def fold_halves(acc, group, width, halves):
    total = fold(acc, group, width)
    rows = total.shape[0] // halves
    return sum(total[half * rows : (half + 1) * rows] for half in range(halves))


def each_chunk(span, chunk_body):
    chunk = span // math.gcd(span // LANE, 9)

    def one(step, carry):
        chunk_body(pl.multiple_of(step * chunk, LANE), chunk)
        return carry

    lax.fori_loop(0, span // chunk, one, 0)


def sums_kernel(
    group, width, halves, x_ref, up_ref, grad_ref, inv_ref, offset_ref, gain_ref,
    mean_ref, cross_ref, gain_grad_ref, shift_grad_ref, ring, inv, offset, acc, acc_cross,
):
    span = group * width
    groups = x_ref.shape[2] // span
    spread_token(inv, ring, inv_ref[0], halves, width)
    spread_token(offset, ring, offset_ref[0], halves, width)

    @pl.when(pl.program_id(0) == 0)
    def _():
        gain_grad_ref[...] = jnp.zeros_like(gain_grad_ref)
        shift_grad_ref[...] = jnp.zeros_like(shift_grad_ref)

    def one(start, chunk):
        here = pl.ds(start, chunk)
        inv_here = inv[:, here]
        offset_here = offset[:, here]
        mean = jnp.zeros((inv.shape[0], chunk), F32)
        cross = jnp.zeros((inv.shape[0], chunk), F32)
        for step in range(groups):
            at = pl.ds(pl.multiple_of(start + step * span, LANE), chunk)
            standard = x_ref[0, :, at].astype(F32) * inv_here - offset_here
            grad = up_ref[0, :, at].astype(F32) + grad_ref[0, :, at].astype(F32)
            gain_grad_ref[:, at] += grad * standard
            shift_grad_ref[:, at] += grad
            grad = grad * gain_ref[:, at]
            mean = mean + grad
            cross = cross + grad * standard
        acc[:, here] = mean
        acc_cross[:, here] = cross

    each_chunk(span, one)
    mean_ref[0] = fold_halves(acc, group, width, halves)
    cross_ref[0] = fold_halves(acc_cross, group, width, halves)


def final_kernel(
    group, width, halves, x_ref, up_ref, grad_ref, inv_ref, slope_ref, level_ref, gain_ref,
    out_ref, ring, inv, slope, level,
):
    span = group * width
    lanes = x_ref.shape[2]
    rows = out_ref.shape[1]
    spread_token(inv, ring, inv_ref[0], halves, width)
    spread_token(slope, ring, slope_ref[0], halves, width)
    spread_token(level, ring, level_ref[0], halves, width)

    def one(start, chunk):
        here = pl.ds(start, chunk)
        inv_here = inv[:, here]
        slope_here = slope[:, here]
        level_here = level[:, here]
        for step in range(lanes // span):
            place = start + step * span
            at = pl.ds(pl.multiple_of(place, LANE), chunk)
            up = up_ref[0, :, at].astype(F32)
            grad = (up + grad_ref[0, :, at].astype(F32)) * gain_ref[:, at]
            out = up + inv_here * grad + (level_here - x_ref[0, :, at].astype(F32) * slope_here)
            for half in range(halves):
                there = pl.ds(pl.multiple_of(place + half * lanes, LANE), chunk)
                out_ref[0, :, there] = out[half * rows : (half + 1) * rows].astype(BF16)

    each_chunk(span, one)


def result_kernel(x_ref, normed_ref, filtered_ref, out_ref):
    out = x_ref[...].astype(F32) + normed_ref[...].astype(F32) + filtered_ref[...].astype(F32)
    out_ref[...] = out.astype(BF16)


def row_call(kernel, name, inputs, kinds, out_kinds, sizes, scratch):
    samples, rows_here, lanes, width, halves = sizes
    many = halves * rows_here
    part = lanes // halves
    shapes = {
        "packed": (samples, many, part),
        "packed_lane": (many, part),
        "field": (samples, rows_here, lanes),
        "token": (samples, rows_here, width),
        "lane": (1, lanes),
        "sum": (many, part),
    }
    specs = {
        "packed": pl.BlockSpec((1, many, part), lambda b: (b, 0, 0)),
        "packed_lane": pl.BlockSpec((many, part), lambda b: (0, 0)),
        "field": pl.BlockSpec((1, rows_here, lanes), lambda b: (b, 0, 0)),
        "token": pl.BlockSpec((1, rows_here, width), lambda b: (b, 0, 0)),
        "lane": pl.BlockSpec((1, lanes), lambda b: (0, 0)),
        "sum": pl.BlockSpec((many, part), lambda b: (0, 0)),
    }
    cells = samples * rows_here * lanes
    return pl.pallas_call(
        kernel,
        grid=(samples,),
        in_specs=[specs[kind] for kind in kinds],
        out_specs=[specs[kind] for kind in out_kinds],
        out_shape=[
            jax.ShapeDtypeStruct(shapes[kind], BF16 if kind == "field" else F32)
            for kind in out_kinds
        ],
        scratch_shapes=scratch,
        compiler_params=pltpu.CompilerParams(vmem_limit_bytes=VMEM_BYTES),
        cost_estimate=pl.CostEstimate(
            flops=cells * 2000, bytes_accessed=2 * cells * (len(kinds) + 1), transcendentals=0
        ),
        name=name,
    )(*inputs)


def swap(values):
    return lax.all_to_all(values, "lat", split_axis=0, concat_axis=0, tiled=True)


def channel_sum(first, second, ch):
    both = jnp.stack((first, second))
    if ch == 2:
        both = both + lax.ppermute(both, "ch", [(0, 1), (1, 0)])
    else:
        both = lax.psum(both, "ch")
    return both[0], both[1]


def wide_matrix(matrix):
    high, low = split_table(matrix)
    return jnp.concatenate((high, high, low), axis=2)


def real_matrix(weight):
    turned = jnp.swapaxes(weight, 2, 3)
    top = jnp.concatenate((turned[0], -turned[1]), axis=2)
    bottom = jnp.concatenate((turned[1], turned[0]), axis=2)
    return jnp.concatenate((top, bottom), axis=1)


def weight_grad(grad, block):
    same = grad[:, :block, :block] + grad[:, block:, block:]
    other = grad[:, block:, :block] - grad[:, :block, block:]
    return jnp.swapaxes(jnp.stack((same, other)), 2, 3)


def bias_rows(bias):
    return jnp.concatenate((bias[0], bias[1]), axis=1)[:, :, None]


def bias_grad(grad, block):
    total = jnp.sum(grad, axis=2)
    return jnp.stack((total[:, :block], total[:, block:]))


def body(
    lat, ch, embed, tokens, norm_gain, norm_shift, first_weight, first_bias, second_weight, second_bias, upstream
):
    samples, rows_here, lanes = tokens.shape
    channels = norm_gain.shape[0]
    width = lanes // channels
    height = rows_here * lat
    block = first_weight.shape[2]
    blocks = first_weight.shape[1]
    group = LANE // math.gcd(width, LANE)
    span = group * width
    halves = 1
    many = halves * rows_here
    part = lanes // halves
    sizes = (samples, rows_here, lanes, width, halves)

    def pack(values):
        pieces = [values[..., half * part : (half + 1) * part] for half in range(halves)]
        return jnp.concatenate(
            [piece.reshape(samples, rows_here, part) for piece in pieces], axis=1
        )

    lat_table = latitude_table(height)
    lon_table, lon_weighted = longitude_table(width)
    lat_forward = left_table(lat_table / math.sqrt(height * width), 2)
    lat_back = left_table(lat_table.T, 1)
    forward_tables = (lat_forward, lat_back, right_table(lon_table, 3), right_table(lon_weighted.T, 1))
    backward_tables = (lat_forward, lat_back, right_table(lon_weighted, 1), right_table(lon_table.T, 1))
    first = real_matrix(first_weight)
    second = real_matrix(second_weight)
    forward_params = (
        wide_matrix(first), bias_rows(first_bias), wide_matrix(second), bias_rows(second_bias),
    )
    backward_params = (
        jnp.swapaxes(first, 1, 2).astype(BF16), jnp.swapaxes(second, 1, 2).astype(BF16),
    )
    gain_lanes = jnp.repeat(norm_gain, width)[None]
    shift_lanes = jnp.repeat(norm_shift, width)[None]
    wide = pltpu.VMEM((rows_here, span), F32)

    early = blocks // 4 * block * width
    upstream_columns = []
    if early:
        upstream_columns.append(swap(upstream[:, :, :early]))
    totals, squares = row_call(
        functools.partial(stats_kernel, group, width), "stats", (tokens,), ("field",),
        ("token", "token"), sizes, [wide, wide],
    )
    totals, squares = channel_sum(totals, squares, ch)
    center = totals / embed
    variance = squares / embed - center * center
    inv_scale = lax.rsqrt(variance + layer_eps)
    (normed,) = row_call(
        functools.partial(norm_kernel, group, width), "norm",
        (tokens, center, inv_scale, gain_lanes, shift_lanes),
        ("field", "token", "token", "lane", "lane"), ("field",), sizes, [wide, wide],
    )
    sent = normed
    if early:
        sent, upstream_columns[0] = lax.optimization_barrier((normed, upstream_columns[0]))
    sent, upstream_late, tokens_late = lax.optimization_barrier((sent, upstream, tokens))
    normed_columns = swap(sent)
    gain_packed = jnp.broadcast_to(
        gain_lanes.reshape(halves, 1, part), (halves, rows_here, part)
    ).reshape(many, part)
    rest, normed_columns, forward_params, backward_params, packs = lax.optimization_barrier(
        (
            upstream_late[:, :, early:], normed_columns, forward_params, backward_params,
            (pack(tokens_late), pack(upstream_late), gain_packed, center * inv_scale),
        )
    )
    tokens_packed, upstream_packed, gain_packed, offset = packs
    upstream_columns.append(swap(rest))
    filtered, *kept = column_forward(
        normed_columns.reshape(height, lanes), forward_tables, forward_params, group, width, block, 0
    )
    filtered, upstream_columns[-1] = lax.optimization_barrier(
        (filtered.reshape(lat, rows_here, lanes), upstream_columns[-1])
    )
    filtered_rows = swap(filtered)
    spectral, first_grad, first_bias_grad, second_grad, second_bias_grad = column_backward(
        jnp.concatenate(upstream_columns, axis=2).reshape(height, lanes), kept,
        backward_tables, backward_params, group, width, block, 0, 0,
    )
    first_all = jnp.concatenate(
        (weight_grad(first_grad, block), bias_grad(first_bias_grad, block)[:, :, None]), axis=2
    )
    second_all = jnp.concatenate(
        (weight_grad(second_grad, block), bias_grad(second_bias_grad, block)[:, :, None]), axis=2
    )
    spectral, filtered_rows, first_all, second_all = lax.optimization_barrier(
        (pack(spectral), filtered_rows, first_all, second_all)
    )
    spectral_rows = swap(spectral)
    (result,) = row_call(
        result_kernel, "result", (tokens, normed, filtered_rows), ("field",) * 3, ("field",), sizes, [],
    )
    first_all, second_all = lax.psum((first_all, second_all), "lat")
    spectral_rows, result = lax.optimization_barrier((spectral_rows, result))
    wide = pltpu.VMEM((many, span), F32)
    ring = pltpu.VMEM((many, 2 * width + LANE), F32)
    mean, cross, gain_part, shift_part = row_call(
        functools.partial(sums_kernel, group, width, halves), "sums",
        (tokens_packed, upstream_packed, spectral_rows, inv_scale, offset, gain_packed),
        ("packed", "packed", "packed", "token", "token", "packed_lane"),
        ("token", "token", "sum", "sum"), sizes, [ring] + [wide] * 4,
    )
    mean, cross = channel_sum(mean, cross, ch)
    mean, first_all, second_all = lax.optimization_barrier((mean, first_all, second_all))
    cross = cross * inv_scale / embed
    (grad_tokens,) = row_call(
        functools.partial(final_kernel, group, width, halves), "final",
        (
            tokens_packed, upstream_packed, spectral_rows, inv_scale, cross * inv_scale,
            cross * offset - mean * inv_scale / embed, gain_packed,
        ),
        ("packed", "packed", "packed", "token", "token", "token", "packed_lane"),
        ("field",), sizes, [ring] + [wide] * 3,
    )
    parts = jnp.stack((gain_part, shift_part)).reshape(2, halves, rows_here, channels // halves, width)
    vector = jnp.broadcast_to(jnp.sum(parts, axis=(2, 4)).reshape(1, 2, channels), (lat, 2, channels))
    gathered = swap(vector)
    gathered, grad_tokens = lax.optimization_barrier((gathered, grad_tokens))
    gain_grad, shift_grad = jnp.sum(gathered, axis=0)
    return (
        result, grad_tokens, first_all[:, :, :block], first_all[:, :, block],
        second_all[:, :, :block], second_all[:, :, block], gain_grad, shift_grad,
    )


def solution(mesh):
    lat = mesh.shape["lat"]
    ch = mesh.shape["ch"]

    def step(tokens, norm_gain, *rest):
        return jax.shard_map(
            functools.partial(body, lat, ch, norm_gain.shape[0]),
            mesh=mesh,
            in_specs=(
                P(None, "lat", "ch"),
                P("ch"),
                P("ch"),
                P(None, "ch", None, None),
                P(None, "ch", None),
                P(None, "ch", None, None),
                P(None, "ch", None),
                P(None, "lat", "ch"),
            ),
            out_specs=(
                P(None, "lat", "ch"),
                P(None, "lat", "ch"),
                P(None, "ch", None, None),
                P(None, "ch", None),
                P(None, "ch", None, None),
                P(None, "ch", None),
                P("ch"),
                P("ch"),
            ),
            check_vma=False,
        )(tokens, norm_gain, *rest)

    return step
```
